256 devices in a mesh: section: 4 (over y_hi, core), img: 64 (over x, z, y_lo).
Axes of the slice: x: 4, y: 4 (y_hi: 2, y_lo: 2; y = y_hi * 2 + y_lo), z: 8, core: 2. Of those that a mesh axis runs over, the one named last changes fastest.
Arguments:
- early_feats: bfloat16 [8, 4096, 1280], P('section', 'img'), may hold values from -6 to 6
- final_embed: bfloat16 [8, 4096, 256], P('section', 'img'), may hold values from -240 to 240
- prompt_counts: int32 [8], replicated, may hold values from 16 to 64, as said below
- box_pixels: int32 [8, 64, 4], replicated, may hold values from 0 to 1023
- pair_table: int32 [8], replicated, may hold values from 0 to 7, as said below
- token_table: float32 [8, 256], replicated, may hold values from -6 to 6
- pe_basis: float32 [2, 128], replicated, may hold values from -5 to 5
- w_early: bfloat16 [1280, 256], replicated, may hold values from -0.15625 to 0.15625
- attend_in: bfloat16 [2, 6, 256, 128], replicated, may hold values from -0.375 to 0.375
- attend_out: bfloat16 [2, 2, 128, 256], replicated, may hold values from -0.5 to 0.5
- mlp_up: bfloat16 [2, 256, 2048], replicated, may hold values from -0.375 to 0.375
- mlp_down: bfloat16 [2, 2048, 256], replicated, may hold values from -0.125 to 0.125
- w_hyper: bfloat16 [256, 256], replicated, may hold values from -0.375 to 0.375
Outputs:
- masks: float32 [8, 64, 4096], P('section', None, 'img')
The draws below stay inside these ranges and needn't reach their ends.
Inputs may be any that keep to these rules, and one draw needn't show every extreme that they name: `prompt_counts`: at least one image has all 64 prompts live. `pair_table`: a permutation of the images that maps all 2 images of an output group to the 2 images of one input group, in any order.
All inputs are finite; a program needn't handle non-finite values.
Results may differ from the reference program's by a relative error of at most 0.017.
The reference program's roundings to bfloat16 on the way count: a program that leaves them out, or rounds other values in their place, can miss the bound.
Values may be sent and summed in bfloat16 or wider, within the bound.
No kernel may reach another device: no remote copies, remote signals or barrier semaphores. Data moves between devices by JAX's collectives and lax.ppermute only.
A program may use at most 64 MiB of HBM per device.

```python
import math
import jax
import jax.numpy as jnp
from jax import lax

D_EARLY = 1280
D = 256
DA = 128
HEADS = 8
MLP = 2048
GRID = 64
IMG_PIX = 1024
PROMPTS = 64
TOKS_P = 8
LAYERS = 2
IMGS = 2
POS = 4096
IMAGES = 8
N_SECTION = 4


def draw_final_embed(key, part):
    key_one, key_two = jax.random.split(jax.random.fold_in(key, 11))
    noise_vals = jnp.clip(jax.random.normal(key_one, (IMAGES, POS, D), jnp.float32), -6.0, 6.0)
    return noise_vals.astype(jnp.bfloat16)


def draw_prompt_counts(key, part):
    key_one, key_two = jax.random.split(jax.random.fold_in(key, 23))
    values = jax.random.randint(key_one, (IMAGES,), PROMPTS // 4, PROMPTS + 1, jnp.int32)
    fullest = jax.random.randint(key_two, (), 0, IMAGES, jnp.int32)
    return jnp.where(jnp.arange(IMAGES, dtype=jnp.int32) == fullest, PROMPTS, values).astype(jnp.int32)


def draw_pair_table(key, part):
    key_one, key_two = jax.random.split(jax.random.fold_in(key, 37))
    group_order = jax.random.permutation(key_one, N_SECTION).astype(jnp.int32)
    scores = jax.random.randint(key_two, (N_SECTION, IMGS), 0, 1 << 20, jnp.int32) * IMGS + jnp.arange(IMGS, dtype=jnp.int32)[None, :]
    inner = jnp.argsort(scores, axis=1).astype(jnp.int32)
    table = group_order[:, None] * IMGS + inner
    return table.reshape(IMAGES).astype(jnp.int32)


def place_ends(drawn, own_key, low, largest):
    extent = drawn.shape
    place = [jax.random.randint(jax.random.fold_in(own_key, axis), (), 0, extent[axis]) for axis in range(len(extent))]
    drawn = drawn.at[tuple(place)].set(low)
    longest = extent.index(max(extent))
    place[longest] = (place[longest] + 1) % extent[longest]
    return drawn.at[tuple(place)].set(largest)


def block_levels(own_key, dims, pieces, smallest, high):
    def one(axis_at, parts):
        draws = jax.random.uniform(jax.random.fold_in(jax.random.fold_in(own_key, 6), axis_at), (parts,), jnp.float32, smallest / len(pieces), high / len(pieces))
        return jnp.repeat(jnp.exp(draws), dims[axis_at] // parts).reshape((-1,) + (1,) * (len(dims) - axis_at - 1))

    level = one(*pieces[0])
    for cut in pieces[1:]:
        level = level * one(*cut)
    return level


def gaussian(rng, dims, scale, reach, cuts=(), held_as=jnp.bfloat16):
    values = scale * jax.random.normal(rng, dims, jnp.float32)
    if cuts:
        values = values * block_levels(rng, dims, cuts, -0.22, 0.18)
    return jnp.clip(values, -reach, reach).astype(held_as)


def setup_inputs(seed: int = 0) -> dict:
    arg_keys = jax.random.split(jax.random.key(seed), 14)
    return {
        "early_feats": gaussian(arg_keys[0], (IMAGES, POS, D_EARLY), 1.0, 6.0, ((0, 4), (1, 64))),
        "final_embed": draw_final_embed(jax.random.fold_in(arg_keys[13], 71), 0),
        "prompt_counts": draw_prompt_counts(jax.random.fold_in(arg_keys[13], 71), 0),
        "box_pixels": place_ends(jax.random.randint(arg_keys[3], (IMAGES, PROMPTS, 4), 0, IMG_PIX), jax.random.fold_in(arg_keys[3], 1), 0, IMG_PIX - 1).astype(jnp.int32),
        "pair_table": draw_pair_table(jax.random.fold_in(arg_keys[13], 71), 0),
        "token_table": gaussian(arg_keys[5], (TOKS_P, D), 1.0, 6.0, (), jnp.float32),
        "pe_basis": gaussian(arg_keys[6], (2, D // 2), 1.0, 5.0, (), jnp.float32),
        "w_early": gaussian(arg_keys[7], (D_EARLY, D), D_EARLY ** -0.5, 0.15625),
        "attend_in": gaussian(arg_keys[8], (LAYERS, 6, D, DA), D ** -0.5, 0.375),
        "attend_out": gaussian(arg_keys[9], (LAYERS, 2, DA, D), DA ** -0.5, 0.5),
        "mlp_up": gaussian(arg_keys[10], (LAYERS, D, MLP), D ** -0.5, 0.375),
        "mlp_down": gaussian(arg_keys[11], (LAYERS, MLP, D), MLP ** -0.5, 0.125),
        "w_hyper": gaussian(arg_keys[12], (D, D), D ** -0.5, 0.375),
    }


NORM_EPS = 0.01

def norm_rows(values):
    center = values - lax.optimization_barrier(jnp.mean(values, axis=-1, keepdims=True))
    spread = lax.optimization_barrier(jnp.mean(center * center, axis=-1, keepdims=True))
    return center / jnp.sqrt(spread + NORM_EPS)

def round_keep(values):
    return lax.optimization_barrier(values.astype(jnp.bfloat16)).astype(jnp.float32)

def fourier(coord_x, coord_y, pe_basis):
    phase = (2.0 * coord_x - 1.0)[..., None] * pe_basis[0] + (2.0 * coord_y - 1.0)[..., None] * pe_basis[1]
    phase = 2.0 * math.pi * phase
    return jnp.concatenate([jnp.sin(phase), jnp.cos(phase)], axis=-1)

def grid_code(index, pe_basis):
    column = (index % GRID).astype(jnp.float32)
    row_idx = (index // GRID).astype(jnp.float32)
    return fourier((column + 0.5) / GRID, (row_idx + 0.5) / GRID, pe_basis)

def start_tokens(box_rows, token_table, pe_basis):
    coords = (box_rows.astype(jnp.float32) + 0.5) / IMG_PIX
    corner_one = fourier(coords[:, 0], coords[:, 1], pe_basis)
    corner_two = fourier(coords[:, 2], coords[:, 3], pe_basis)
    slots = jnp.arange(TOKS_P)[None, :, None]
    tokens = token_table[None] + jnp.where(slots == TOKS_P - 2, corner_one[:, None, :], 0.0)
    tokens = tokens + jnp.where(slots == TOKS_P - 1, corner_two[:, None, :], 0.0)
    return tokens.reshape(-1, token_table.shape[-1])

def attend(queries, keys, values, live):
    query_rows = queries.shape[0]
    key_rows = keys.shape[0]
    head_size = queries.shape[1] // HEADS
    query_heads = queries.reshape(query_rows, HEADS, head_size).astype(jnp.float32)
    key_heads = keys.reshape(key_rows, HEADS, head_size).astype(jnp.float32)
    scores = jnp.einsum('qhd,khd->hqk', query_heads, key_heads) * head_size ** (-0.5)
    if live is not None:
        scores = jnp.where(live[None, None, :], scores, -jnp.inf)
    highest = lax.optimization_barrier(jnp.max(scores, axis=-1, keepdims=True))
    weights = round_keep(jnp.exp(scores - highest))
    value_heads = values.reshape(key_rows, HEADS, head_size).astype(jnp.float32)
    summed = jnp.einsum('hqk,khd->qhd', weights, value_heads)
    totals = lax.optimization_barrier(jnp.sum(weights, axis=-1))
    return (summed / jnp.transpose(totals)[:, :, None]).reshape(query_rows, HEADS * head_size)

def bdot(left, right):
    return jnp.dot(left, right, preferred_element_type=jnp.float32)

def decode(early_one, final_one, count_one, boxes_one, token_table, pe_basis, w_early, attend_in, attend_out, mlp_up, mlp_down, w_hyper):
    hq_part = round_keep(jax.nn.gelu(bdot(early_one, w_early), approximate=False))
    img_code = grid_code(jnp.arange(POS, dtype=jnp.int32), pe_basis)
    image = final_one.astype(jnp.float32)
    tokens = start_tokens(boxes_one, token_table, pe_basis)
    live_prompt = jnp.arange(PROMPTS, dtype=jnp.int32) < count_one
    live_token = jnp.repeat(live_prompt, TOKS_P)
    token_bf = tokens.astype(jnp.bfloat16)
    for layer in range(LAYERS):
        token_bf = tokens.astype(jnp.bfloat16)
        image_bf = image.astype(jnp.bfloat16)
        key_bf = (image + img_code).astype(jnp.bfloat16)
        query_one = bdot(token_bf, attend_in[layer, 0]).astype(jnp.bfloat16)
        keys_one = bdot(key_bf, attend_in[layer, 1]).astype(jnp.bfloat16)
        values_one = bdot(image_bf, attend_in[layer, 2]).astype(jnp.bfloat16)
        first_out = attend(query_one, keys_one, values_one, None)
        tok_two = norm_rows(tokens + bdot(first_out.astype(jnp.bfloat16), attend_out[layer, 0]))
        hidden = jax.nn.relu(bdot(tok_two.astype(jnp.bfloat16), mlp_up[layer])).astype(jnp.bfloat16)
        tok_three = norm_rows(tok_two + bdot(hidden, mlp_down[layer]))
        token_bf = tok_three.astype(jnp.bfloat16)
        query_two = bdot(key_bf, attend_in[layer, 3]).astype(jnp.bfloat16)
        keys_two = bdot(token_bf, attend_in[layer, 4]).astype(jnp.bfloat16)
        values_two = bdot(token_bf, attend_in[layer, 5]).astype(jnp.bfloat16)
        second_out = attend(query_two, keys_two, values_two, live_token)
        image = norm_rows(image + bdot(second_out.astype(jnp.bfloat16), attend_out[layer, 1]))
        tokens = tok_three
    hq_rows = token_bf.reshape(PROMPTS, TOKS_P, -1)[:, TOKS_P - 3]
    hyper = bdot(hq_rows, w_hyper).astype(jnp.bfloat16)
    mask_feats = (image + hq_part).astype(jnp.bfloat16)
    logits = bdot(hyper, jnp.transpose(mask_feats)) * D ** (-0.5)
    return jnp.where(live_prompt[:, None], logits, 0.0)

def reference(early_feats, final_embed, prompt_counts, box_pixels, pair_table, token_table, pe_basis, w_early, attend_in, attend_out, mlp_up, mlp_down, w_hyper):

    def one_image(index):
        picked = pair_table[index].astype(jnp.int32)
        return decode(early_feats[picked], final_embed[picked], prompt_counts[picked], box_pixels[picked], token_table, pe_basis, w_early, attend_in, attend_out, mlp_up, mlp_down, w_hyper)
    return lax.map(one_image, jnp.arange(IMAGES, dtype=jnp.int32))
```

```python
import math

import jax
import jax.numpy as jnp
from jax import lax
from jax.sharding import Mesh
from jax.sharding import PartitionSpec as P

HEADS = 8
GRID = 64
IMG_PIX = 1024
TOKS_P = 8
LAYERS = 2
NORM_EPS = 0.01
SPLIT = ("section", "x", "zh", "zl", "y")
IMG = ("x", "zh", "zl", "y")
bf16 = jnp.bfloat16
f32 = jnp.float32


def bdot(left, right):
    return jnp.dot(left, right, preferred_element_type=f32)


def norm_rows(values):
    center = values - jnp.mean(values, axis=-1, keepdims=True)
    spread = jnp.mean(center * center, axis=-1, keepdims=True)
    return center / jnp.sqrt(spread + NORM_EPS)


def swapped(x, axis, distance):
    return lax.ppermute(x, axis, [(i, i ^ distance) for i in range(lax.axis_size(axis))])


def fourier(coord_x, coord_y, pe_basis):
    phase = (2.0 * coord_x - 1.0)[..., None] * pe_basis[0] + (2.0 * coord_y - 1.0)[
        ..., None
    ] * pe_basis[1]
    phase = 2.0 * math.pi * phase
    return jnp.concatenate([jnp.sin(phase), jnp.cos(phase)], axis=-1)


def grid_code(grid_rows, pe_basis):
    column = (jnp.arange(GRID, dtype=f32) + 0.5) / GRID
    row = (grid_rows.astype(f32) + 0.5) / GRID
    a = 2.0 * math.pi * (2.0 * column - 1.0)[:, None] * pe_basis[0]
    b = 2.0 * math.pi * (2.0 * row - 1.0)[:, None] * pe_basis[1]
    sa, ca = jnp.sin(a)[None], jnp.cos(a)[None]
    sb, cb = jnp.sin(b)[:, None], jnp.cos(b)[:, None]
    code = jnp.concatenate([sa * cb + ca * sb, ca * cb - sa * sb], axis=-1)
    return code.reshape(-1, code.shape[-1])


def start_tokens(box_rows, token_table, pe_basis):
    coords = (box_rows.astype(f32) + 0.5) / IMG_PIX
    corner_one = fourier(coords[:, 0], coords[:, 1], pe_basis)
    corner_two = fourier(coords[:, 2], coords[:, 3], pe_basis)
    slots = jnp.arange(TOKS_P)[None, :, None]
    tokens = token_table[None] + jnp.where(slots == TOKS_P - 2, corner_one[:, None, :], 0.0)
    tokens = tokens + jnp.where(slots == TOKS_P - 1, corner_two[:, None, :], 0.0)
    return tokens.reshape(-1, token_table.shape[-1])


def pieces(v):
    hi = lax.reduce_precision(v, 8, 7)
    rest = v - hi
    mid = lax.reduce_precision(rest, 8, 7)
    low = rest - mid
    return [hi.astype(bf16), mid.astype(bf16), low.astype(bf16)]


def partial_attend(query, keys, values):
    toks, width = query.shape
    size = width // HEADS
    scores = jnp.einsum(
        "khd,qhd->hkq",
        keys.reshape(-1, HEADS, size),
        query.reshape(-1, HEADS, size),
        preferred_element_type=f32,
    ) * size ** (-0.5)
    top = jnp.max(scores, axis=1)
    weights = jnp.exp(scores - top[:, None]).astype(bf16)
    summed = jnp.einsum(
        "hkq,khd->hdq", weights, values.reshape(-1, HEADS, size), preferred_element_type=f32
    )
    total = jnp.sum(weights.astype(f32), axis=1)
    return jnp.concatenate(
        [summed.reshape(width, toks).astype(bf16), total.astype(bf16)] + pieces(top), axis=0
    )


def combined(parts):
    width = parts.shape[1] - 4 * HEADS
    parts = parts.astype(f32)
    summed, total = parts[:, :width], parts[:, width : width + HEADS]
    hi, mid, low = (
        parts[:, width + (k + 1) * HEADS : width + (k + 2) * HEADS] for k in range(3)
    )
    top = hi + (mid + low)
    share = jnp.exp(top - jnp.max(top, axis=0, keepdims=True))
    size = width // HEADS
    total = jnp.sum(total * share, axis=0)
    summed = jnp.sum(summed.reshape(-1, HEADS, size, summed.shape[-1]) * share[:, :, None], axis=0)
    return (summed / total[:, None]).reshape(width, -1).T


def token_step(parts, tok, out_w, up, down):
    first = combined(parts)
    two = norm_rows(tok + bdot(first.astype(bf16), out_w))
    hidden = jax.nn.relu(bdot(two.astype(bf16), up)).astype(bf16)
    return norm_rows(two + bdot(hidden, down))


def image_step(image, key_bf, toks, live, w_q, w_k, w_v, w_o):
    query = bdot(key_bf, w_q).astype(bf16)
    keys = bdot(toks, w_k).astype(bf16)
    values = bdot(toks, w_v).astype(bf16)
    size = query.shape[1] // HEADS
    scores = jnp.einsum(
        "qhd,khd->hqk",
        query.reshape(-1, HEADS, size),
        keys.reshape(-1, HEADS, size),
        preferred_element_type=f32,
    ) * size ** (-0.5)
    scores = jnp.where(live[None, None, :], scores, -jnp.inf)
    top = jnp.max(scores, axis=-1, keepdims=True)
    weights = jnp.exp(scores - top).astype(bf16)
    summed = jnp.einsum(
        "hqk,khd->qhd", weights, values.reshape(-1, HEADS, size), preferred_element_type=f32
    )
    total = jnp.sum(weights.astype(f32), axis=-1).T
    second = (summed / total[:, :, None]).reshape(query.shape)
    return norm_rows(image + bdot(second.astype(bf16), w_o))


def shards(
    early_feats,
    final_embed,
    prompt_counts,
    box_pixels,
    pair_table,
    token_table,
    pe_basis,
    w_early,
    attend_in,
    attend_out,
    mlp_up,
    mlp_down,
    w_hyper,
):
    images, pos_dev, width = final_embed.shape
    prompts = box_pixels.shape[1]
    n_x, n_zh, n_zl, n_y = (lax.axis_size(a) for a in IMG)
    section = lax.axis_index("section")
    my_x, my_zh, my_zl, my_y = (lax.axis_index(a) for a in IMG)
    mine = section * images + my_y

    sent = jnp.broadcast_to(final_embed[None], (n_x * n_zh,) + final_embed.shape)
    sent = sent.reshape(n_x * n_zh * n_y, pos_dev, width)
    held = lax.all_to_all(sent, ("x", "zh", "y"), 0, 0, tiled=True)
    image = held.reshape(-1, width).astype(f32)

    hq = jax.nn.gelu(bdot(early_feats, w_early), approximate=False).astype(bf16)
    hq_keep = lax.dynamic_index_in_dim(hq, my_y, 0, keepdims=False)
    hq_send = lax.dynamic_index_in_dim(hq, 1 - my_y, 0, keepdims=False)
    hq_got = swapped(hq_send, "y", 1)
    hq_here = jnp.where(
        my_y == 0,
        jnp.concatenate([hq_keep, hq_got], axis=0),
        jnp.concatenate([hq_got, hq_keep], axis=0),
    )

    ids = jnp.arange(n_x * n_zh * n_y, dtype=jnp.int32)
    grid_rows = (ids // 4) * (n_zh * n_zl * n_y) + (ids // 2 % 2) * (n_zl * n_y)
    grid_rows = grid_rows + my_zl * n_y + ids % 2
    code = grid_code(grid_rows, pe_basis)
    count = prompt_counts[mine]
    boxes = lax.dynamic_index_in_dim(box_pixels, mine, 0, keepdims=False)
    own_prompts = prompts // n_x
    boxes = lax.dynamic_slice_in_dim(boxes, my_x * own_prompts, own_prompts, 0)
    tok = start_tokens(boxes, token_table, pe_basis)
    live_prompt = jnp.arange(prompts, dtype=jnp.int32) < count
    live = jnp.repeat(live_prompt, TOKS_P)
    tok_b = tok.astype(bf16)
    own_pos = n_y * pos_dev
    for layer in range(LAYERS):
        w = attend_in[layer]
        image_bf = image.astype(bf16)
        key_bf = (image + code).astype(bf16)
        query = bdot(tok_b, w[0]).astype(bf16)
        keys = bdot(key_bf, w[1]).astype(bf16)
        values = bdot(image_bf, w[2]).astype(bf16)
        part = partial_attend(query, keys, values)
        parts = jnp.stack([part] + [swapped(part, "zl", d) for d in range(1, n_zl)])
        tok = token_step(parts, tok, attend_out[layer, 0], mlp_up[layer], mlp_down[layer])
        tok_b = tok.astype(bf16)
        got = jnp.stack([tok_b] + [swapped(tok_b, "x", d) for d in range(1, n_x)])
        toks = jnp.take(got, jnp.arange(n_x, dtype=jnp.int32) ^ my_x, axis=0).reshape(-1, width)
        if layer == LAYERS - 1:
            start = (my_x * n_zh + my_zh) * own_pos
            image = lax.dynamic_slice_in_dim(image, start, own_pos, 0)
            key_bf = lax.dynamic_slice_in_dim(key_bf, start, own_pos, 0)
        image = image_step(image, key_bf, toks, live, w[3], w[4], w[5], attend_out[layer, 1])
    hyper = bdot(toks.reshape(-1, TOKS_P, width)[:, TOKS_P - 3], w_hyper).astype(bf16)
    feats = (image + hq_here.astype(f32)).astype(bf16)
    logits = lax.dot_general(
        hyper, feats, (((1,), (1,)), ((), ())), preferred_element_type=f32
    ) * width ** (-0.5)
    masks = jnp.where(live_prompt[:, None], logits, 0.0)

    halves = [masks[:, :pos_dev], masks[:, pos_dev:]]
    keep = jnp.where(my_y == 0, halves[0], halves[1])
    give = jnp.where(my_y == 0, halves[1], halves[0])
    got = swapped(give, "y", 1)
    both = jnp.where(my_y == 0, jnp.stack([keep, got]), jnp.stack([got, keep]))
    every = jnp.stack(
        [both] + [swapped(both, "section", d) for d in range(1, lax.axis_size("section"))]
    )
    table = lax.dynamic_slice_in_dim(pair_table, section * images, images, 0)
    chosen = lax.dynamic_index_in_dim(every, (table[0] // images) ^ section, 0, keepdims=False)
    swap = (table[0] % images) == 1
    return jnp.where(swap, chosen[::-1], chosen)


def solution(mesh):
    n_sec, n_img = mesh.devices.shape
    fine = Mesh(mesh.devices.reshape(n_sec, 4, 2, 4, 2), SPLIT)
    placed = (P("section", IMG, None),) * 2 + (P(),) * 11
    return jax.shard_map(
        shards, mesh=fine, in_specs=placed, out_specs=P("section", None, IMG), check_vma=False
    )
```

```python
import math

import jax
import jax.numpy as jnp
from jax import lax
from jax.experimental import pallas as pl
from jax.experimental.pallas import tpu as pltpu
from jax.sharding import Mesh
from jax.sharding import PartitionSpec as P

HEADS = 8
GRID = 64
IMG_PIX = 1024
TOKS_P = 8
NORM_EPS = 0.01
SPLIT = ("section", "x", "zh", "zl", "y")
IMG = ("x", "zh", "zl", "y")
bf16 = jnp.bfloat16
f32 = jnp.float32


def bdot(left, right):
    return jnp.dot(left, right, preferred_element_type=f32)


def norm_rows(values):
    center = values - jnp.mean(values, axis=-1, keepdims=True)
    spread = jnp.mean(center * center, axis=-1, keepdims=True)
    return center / jnp.sqrt(spread + NORM_EPS)


def swapped(x, axis, distance):
    return lax.ppermute(x, axis, [(i, i ^ distance) for i in range(lax.axis_size(axis))])


def fourier(coord_x, coord_y, pe_basis):
    phase = (2.0 * coord_x - 1.0)[..., None] * pe_basis[0] + (2.0 * coord_y - 1.0)[
        ..., None
    ] * pe_basis[1]
    phase = 2.0 * math.pi * phase
    return jnp.concatenate([jnp.sin(phase), jnp.cos(phase)], axis=-1)


def grid_tables(grid_rows, pe_basis):
    column = (jnp.arange(GRID, dtype=f32) + 0.5) / GRID
    row = (grid_rows.astype(f32) + 0.5) / GRID
    a = 2.0 * math.pi * (2.0 * column - 1.0)[:, None] * pe_basis[0]
    b = 2.0 * math.pi * (2.0 * row - 1.0)[:, None] * pe_basis[1]
    return (
        jnp.concatenate([jnp.sin(a), jnp.cos(a)], axis=-1),
        jnp.concatenate([jnp.sin(b), jnp.cos(b)], axis=-1),
    )


def start_tokens(box_rows, token_table, pe_basis):
    coords = (box_rows.astype(f32) + 0.5) / IMG_PIX
    corner_one = fourier(coords[:, 0], coords[:, 1], pe_basis)
    corner_two = fourier(coords[:, 2], coords[:, 3], pe_basis)
    slots = jnp.arange(TOKS_P)[None, :, None]
    tokens = token_table[None] + jnp.where(slots == TOKS_P - 2, corner_one[:, None, :], 0.0)
    tokens = tokens + jnp.where(slots == TOKS_P - 1, corner_two[:, None, :], 0.0)
    return tokens.reshape(-1, token_table.shape[-1])


def dot_at(left, right, l_dim, r_dim):
    return lax.dot_general(
        left, right, (((l_dim,), (r_dim,)), ((), ())), preferred_element_type=f32
    )


def code_rows(cols_ref, rows_ref, row, count):
    half = cols_ref.shape[1] // 2
    sa, ca = cols_ref[:, :half], cols_ref[:, half:]
    out = []
    for k in range(count):
        sb = rows_ref[row + k][:, :half]
        cb = rows_ref[row + k][:, half:]
        out.append(jnp.concatenate([sa * cb + ca * sb, ca * cb - sa * sb], axis=1))
    return jnp.concatenate(out, axis=0)


def one_head(values, head, size):
    lane = lax.broadcasted_iota(jnp.int32, values.shape, 1)
    return jnp.where(lane // size == head, values, jnp.zeros_like(values))


def pieces(v):
    hi = v.astype(bf16)
    rest = v - hi.astype(f32)
    mid = rest.astype(bf16)
    low = (rest - mid.astype(f32)).astype(bf16)
    return [hi, mid, low]


def partial_attend(query, key_ref, image_ref, w_k, w_v, out_ref):
    width = w_k.shape[1]
    size = width // HEADS
    query = (query * size ** (-0.5)).astype(bf16)
    keys = bdot(key_ref[...], w_k).astype(bf16)
    values = dot_at(w_v, image_ref[...], 0, 1).astype(bf16)
    ones = jnp.ones((size, values.shape[1]), bf16)
    totals, tops = [], []
    for head in range(HEADS):
        scores = dot_at(keys, one_head(query, head, size), 1, 1)
        top = jnp.max(scores, axis=0, keepdims=True)
        weights = jnp.exp(scores - top).astype(bf16)
        own = values[head * size : (head + 1) * size]
        both = bdot(jnp.concatenate([own, ones], axis=0), weights)
        out_ref[head * size : (head + 1) * size, :] = both[:size].astype(bf16)
        totals.append(both[size : size + 1])
        tops.append(top)
    total = jnp.concatenate(totals, axis=0)
    tops = pieces(jnp.concatenate(tops, axis=0))
    tail = jnp.concatenate([total] + [t.astype(f32) for t in tops], axis=0)
    out_ref[width:, :] = tail.astype(bf16)


def first_kernel(tok_ref, image_ref, cols_ref, rows_ref, w_ref, out_ref, key_ref):
    step = 4
    for k in range(0, rows_ref.shape[0], step):
        at = slice(k * GRID, (k + step) * GRID)
        code = code_rows(cols_ref, rows_ref, k, step)
        key_ref[at, :] = (image_ref[at, :].astype(f32) + code).astype(bf16)
    query = bdot(tok_ref[...].astype(bf16), w_ref[0]).astype(bf16)
    partial_attend(query.astype(f32), key_ref, image_ref, w_ref[1], w_ref[2], out_ref)


def token_kernel(p0, p1, p2, p3, tok_ref, w_ref, up_ref, down_ref, out_ref, short_ref):
    refs = (p0, p1, p2, p3)
    width = w_ref.shape[0]
    size = width // HEADS
    tails = [r[width:, :].astype(f32) for r in refs]
    tops = [t[HEADS : 2 * HEADS] + (t[2 * HEADS : 3 * HEADS] + t[3 * HEADS :]) for t in tails]
    peak = jnp.maximum(jnp.maximum(tops[0], tops[1]), jnp.maximum(tops[2], tops[3]))
    shares = [jnp.exp(t - peak) for t in tops]
    total = sum(t[:HEADS] * s for t, s in zip(tails, shares))
    heads = []
    for head in range(HEADS):
        at = slice(head * size, (head + 1) * size)
        row = slice(head, head + 1)
        summed = sum(r[at, :].astype(f32) * s[row] for r, s in zip(refs, shares))
        heads.append(summed / total[row])
    first = jnp.concatenate(heads, axis=0).astype(bf16)
    two = norm_rows(tok_ref[...] + dot_at(first, w_ref[...], 0, 0))
    hidden = jnp.maximum(bdot(two.astype(bf16), up_ref[...]), 0.0).astype(bf16)
    three = norm_rows(two + bdot(hidden, down_ref[...]))
    out_ref[...] = three
    short_ref[...] = three.astype(bf16)


def token_sides(tok_refs, scal_ref, w_k, w_v, k_ref, v_ref):
    width = w_k.shape[1]
    toks = tok_refs[0].shape[0]
    for k, ref in enumerate(tok_refs):
        at = slice(k * toks, (k + 1) * toks)
        tok = ref[...]
        first = (scal_ref[0] ^ k) * toks
        k_ref[at, :width] = bdot(tok, w_k).astype(bf16)
        row = lax.broadcasted_iota(jnp.int32, (toks, width), 0) + first
        lane = lax.broadcasted_iota(jnp.int32, (toks, width), 1)
        dead = (row >= scal_ref[1] * TOKS_P) & (lane == 0)
        k_ref[at, width:] = jnp.where(dead, -1e30, 0.0).astype(bf16)
        v_ref[:, at] = dot_at(w_v, tok, 0, 1).astype(bf16)


def image_attend(key, w_q, w_o, k_ref, v_ref):
    width = w_q.shape[1]
    size = width // HEADS
    query = bdot(key, w_q).astype(bf16).astype(f32) * size ** (-0.5)
    lane = lax.broadcasted_iota(jnp.int32, query.shape, 1)
    query = jnp.concatenate([query, jnp.where(lane == 0, 1.0, 0.0)], axis=1).astype(bf16)
    ones = jnp.ones((size, v_ref.shape[1]), bf16)
    heads = []
    for head in range(HEADS):
        keys = jnp.concatenate(
            [one_head(k_ref[:, :width], head, size), k_ref[:, width:]], axis=1
        )
        scores = dot_at(keys, query, 1, 1)
        top = jnp.max(scores, axis=0, keepdims=True)
        weights = jnp.exp(scores - top).astype(bf16)
        own = v_ref[head * size : (head + 1) * size, :]
        both = bdot(jnp.concatenate([own, ones], axis=0), weights)
        heads.append(both[:size] / both[size : size + 1])
    second = jnp.concatenate(heads, axis=0).astype(bf16)
    return dot_at(second, w_o, 0, 0)


def middle_kernel(
    scal_ref, t0, t1, t2, t3, image_ref, cols_ref, rows_ref, w_ref, next_ref, o_ref,
    out_ref, own_ref, own_key_ref, k_ref, v_ref, key_ref, new_ref, full_ref,
):
    token_sides((t0, t1, t2, t3), scal_ref, w_ref[4], w_ref[5], k_ref, v_ref)
    step = 4
    chunk = step * GRID

    def one(c, carry):
        at = pl.ds(pl.multiple_of(c * chunk, chunk), chunk)
        code = code_rows(cols_ref, rows_ref, c * step, step)
        image = image_ref[at, :].astype(f32)
        key = (image + code).astype(bf16)
        image = norm_rows(image + image_attend(key, w_ref[3], o_ref[...], k_ref, v_ref))
        full_ref[at, :] = image
        new_ref[at, :] = image.astype(bf16)
        key_ref[at, :] = (image + code).astype(bf16)
        return carry

    lax.fori_loop(0, image_ref.shape[0] // chunk, one, 0)
    own = pl.ds(pl.multiple_of(scal_ref[2], own_ref.shape[0]), own_ref.shape[0])
    own_ref[...] = full_ref[own, :]
    own_key_ref[...] = key_ref[own, :]
    query = bdot(t0[...], next_ref[0]).astype(bf16)
    partial_attend(query.astype(f32), key_ref, new_ref, next_ref[1], next_ref[2], out_ref)


def last_kernel(
    scal_ref, t0, t1, t2, t3, image_ref, key_ref, w_ref, o_ref, hq_ref, hyper_ref,
    out_ref, k_ref, v_ref, logit_ref,
):
    refs = (t0, t1, t2, t3)
    token_sides(refs, scal_ref, w_ref[4], w_ref[5], k_ref, v_ref)
    image = image_ref[...]
    image = norm_rows(
        image + image_attend(key_ref[...], w_ref[3], o_ref[...], k_ref, v_ref)
    )
    feats = (image + hq_ref[...].astype(f32)).astype(bf16)
    scale = image.shape[1] ** (-0.5)
    toks = t0.shape[0]
    prompts = toks // TOKS_P
    for k, ref in enumerate(refs):
        hyper = bdot(ref[...], hyper_ref[...]).astype(bf16)
        logit_ref[...] = dot_at(hyper, feats, 1, 1) * scale
        rows = logit_ref[pl.ds(TOKS_P - 3, prompts, stride=TOKS_P), :]
        first = (scal_ref[0] ^ k) * prompts
        live = lax.broadcasted_iota(jnp.int32, rows.shape, 0) + first < scal_ref[1]
        out_ref[pl.ds(pl.multiple_of(first, prompts), prompts), :] = jnp.where(live, rows, 0.0)


def call(kernel, name, outs, scratch=(), scalars=0):
    vmem = pl.BlockSpec(memory_space=pltpu.VMEM)

    def run(*args):
        specs = [pl.BlockSpec(memory_space=pltpu.SMEM)] * scalars
        specs += [vmem] * (len(args) - scalars)
        return pl.pallas_call(
            kernel,
            out_shape=[jax.ShapeDtypeStruct(s, d) for s, d in outs],
            in_specs=specs,
            out_specs=[vmem] * len(outs),
            scratch_shapes=[pltpu.VMEM(s, d) for s, d in scratch],
            compiler_params=pltpu.CompilerParams(vmem_limit_bytes=48 * 2**20),
            name=name,
        )(*args)

    return run


def shards(
    early_feats,
    final_embed,
    prompt_counts,
    box_pixels,
    pair_table,
    token_table,
    pe_basis,
    w_early,
    attend_in,
    attend_out,
    mlp_up,
    mlp_down,
    w_hyper,
):
    images, pos_dev, width = final_embed.shape
    prompts = box_pixels.shape[1]
    n_x, n_zh, n_zl, n_y = (lax.axis_size(a) for a in IMG)
    section = lax.axis_index("section")
    my_x, my_zh, my_zl, my_y = (lax.axis_index(a) for a in IMG)
    mine = section * images + my_y

    sent = jnp.broadcast_to(final_embed[None], (n_x * n_zh,) + final_embed.shape)
    sent = sent.reshape(n_x * n_zh * n_y, pos_dev, width)
    held = lax.all_to_all(sent, ("x", "zh", "y"), 0, 0, tiled=True)
    image = held.reshape(-1, width)

    hq = jax.nn.gelu(bdot(early_feats, w_early), approximate=False).astype(bf16)
    hq_keep = lax.dynamic_index_in_dim(hq, my_y, 0, keepdims=False)
    hq_send = lax.dynamic_index_in_dim(hq, 1 - my_y, 0, keepdims=False)
    hq_got = swapped(hq_send, "y", 1)
    hq_here = jnp.where(
        my_y == 0,
        jnp.concatenate([hq_keep, hq_got], axis=0),
        jnp.concatenate([hq_got, hq_keep], axis=0),
    )

    ids = jnp.arange(n_x * n_zh * n_y, dtype=jnp.int32)
    grid_rows = (ids // 4) * (n_zh * n_zl * n_y) + (ids // 2 % 2) * (n_zl * n_y)
    grid_rows = grid_rows + my_zl * n_y + ids % 2
    cols, rows = grid_tables(grid_rows, pe_basis)
    rows = rows[:, None]
    count = prompt_counts[mine]
    boxes = lax.dynamic_index_in_dim(box_pixels, mine, 0, keepdims=False)
    own_prompts = prompts // n_x
    boxes = lax.dynamic_slice_in_dim(boxes, my_x * own_prompts, own_prompts, 0)
    tok = start_tokens(boxes, token_table, pe_basis)
    own_pos = n_y * pos_dev
    scal = jnp.stack([my_x, count, (my_x * n_zh + my_zh) * own_pos]).astype(jnp.int32)
    n_tok, n_pos, att = tok.shape[0], image.shape[0], attend_in.shape[-1]
    packed = ((att + 4 * HEADS, n_tok), bf16)
    sides = [((n_x * n_tok, 2 * att), bf16), ((att, n_x * n_tok), bf16)]

    def token_step(part, tok, layer):
        parts = [part] + [swapped(part, "zl", d) for d in range(1, n_zl)]
        outs = [(tok.shape, f32), (tok.shape, bf16)]
        tok, short = call(token_kernel, "tokens", outs)(
            *parts, tok, attend_out[layer, 0], mlp_up[layer], mlp_down[layer]
        )
        return tok, [short] + [swapped(short, "x", d) for d in range(1, n_x)]

    (part,) = call(first_kernel, "first", [packed], [((n_pos, width), bf16)])(
        tok, image, cols, rows, attend_in[0]
    )
    tok, toks = token_step(part, tok, 0)
    part, own, own_key = call(
        middle_kernel,
        "middle",
        [packed, ((own_pos, width), f32), ((own_pos, width), bf16)],
        sides + [((n_pos, width), d) for d in (bf16, bf16, f32)],
        1,
    )(scal, *toks, image, cols, rows, attend_in[0], attend_in[1], attend_out[0, 1])
    tok, toks = token_step(part, tok, 1)
    (masks,) = call(
        last_kernel,
        "last",
        [((prompts, own_pos), f32)],
        sides + [((n_tok, own_pos), f32)],
        1,
    )(scal, *toks, own, own_key, attend_in[1], attend_out[1, 1], hq_here, w_hyper)

    halves = [masks[:, :pos_dev], masks[:, pos_dev:]]
    keep = jnp.where(my_y == 0, halves[0], halves[1])
    give = jnp.where(my_y == 0, halves[1], halves[0])
    got = swapped(give, "y", 1)
    both = jnp.where(my_y == 0, jnp.stack([keep, got]), jnp.stack([got, keep]))
    every = jnp.stack(
        [both] + [swapped(both, "section", d) for d in range(1, lax.axis_size("section"))]
    )
    table = lax.dynamic_slice_in_dim(pair_table, section * images, images, 0)
    chosen = lax.dynamic_index_in_dim(every, (table[0] // images) ^ section, 0, keepdims=False)
    swap = (table[0] % images) == 1
    return jnp.where(swap, chosen[::-1], chosen)


def solution(mesh):
    n_sec, n_img = mesh.devices.shape
    fine = Mesh(mesh.devices.reshape(n_sec, 4, 2, 4, 2), SPLIT)
    placed = (P("section", IMG, None),) * 2 + (P(),) * 11
    return jax.shard_map(
        shards, mesh=fine, in_specs=placed, out_specs=P("section", None, IMG), check_vma=False
    )
```

```python
import functools
import math

import jax
import jax.numpy as jnp
from jax import lax
from jax.experimental import pallas as pl
from jax.experimental.pallas import tpu as pltpu
from jax.sharding import Mesh
from jax.sharding import PartitionSpec as P

HEADS = 8
GRID = 64
IMG_PIX = 1024
TOKS_P = 8
NORM_EPS = 0.01
A1_AHEAD = 4
SPLIT = ("section", "x", "zh", "zl", "y")
IMG = ("x", "zh", "zl", "y")
bf16 = jnp.bfloat16
f32 = jnp.float32


def bdot(left, right):
    return jnp.dot(left, right, preferred_element_type=f32)


def norm_rows(values):
    center = values - jnp.mean(values, axis=-1, keepdims=True)
    spread = jnp.mean(center * center, axis=-1, keepdims=True)
    return center / jnp.sqrt(spread + NORM_EPS)


def swapped(x, axis, distance):
    return lax.ppermute(x, axis, [(i, i ^ distance) for i in range(lax.axis_size(axis))])


def fourier(coord_x, coord_y, pe_basis):
    phase = (2.0 * coord_x - 1.0)[..., None] * pe_basis[0] + (2.0 * coord_y - 1.0)[
        ..., None
    ] * pe_basis[1]
    phase = 2.0 * math.pi * phase
    return jnp.concatenate([jnp.sin(phase), jnp.cos(phase)], axis=-1)


def grid_tables(grid_rows, pe_basis):
    column = (jnp.arange(GRID, dtype=f32) + 0.5) / GRID
    row = (grid_rows.astype(f32) + 0.5) / GRID
    a = 2.0 * math.pi * (2.0 * column - 1.0)[:, None] * pe_basis[0]
    b = 2.0 * math.pi * (2.0 * row - 1.0)[:, None] * pe_basis[1]
    return (
        jnp.concatenate([jnp.sin(a), jnp.cos(a)], axis=-1),
        jnp.concatenate([jnp.sin(b), jnp.cos(b)], axis=-1),
    )


def start_tokens(box_rows, token_table, pe_basis):
    coords = (box_rows.astype(f32) + 0.5) / IMG_PIX
    corner_one = fourier(coords[:, 0], coords[:, 1], pe_basis)
    corner_two = fourier(coords[:, 2], coords[:, 3], pe_basis)
    slots = jnp.arange(TOKS_P)[None, :, None]
    tokens = token_table[None] + jnp.where(slots == TOKS_P - 2, corner_one[:, None, :], 0.0)
    tokens = tokens + jnp.where(slots == TOKS_P - 1, corner_two[:, None, :], 0.0)
    return tokens.reshape(-1, token_table.shape[-1])


def dot_at(left, right, l_dim, r_dim):
    return lax.dot_general(
        left, right, (((l_dim,), (r_dim,)), ((), ())), preferred_element_type=f32
    )


def code_rows(cols_ref, rows_ref, row, count):
    half = cols_ref.shape[1] // 2
    sa, ca = cols_ref[:, :half], cols_ref[:, half:]
    out = []
    for k in range(count):
        sb = rows_ref[row + k][:, :half]
        cb = rows_ref[row + k][:, half:]
        out.append(jnp.concatenate([sa * cb + ca * sb, ca * cb - sa * sb], axis=1))
    return jnp.concatenate(out, axis=0)


def one_head(values, head, size):
    lane = lax.broadcasted_iota(jnp.int32, values.shape, 1)
    return jnp.where(lane // size == head, values, jnp.zeros_like(values))


def pieces(v):
    hi = v.astype(bf16)
    rest = v - hi.astype(f32)
    mid = rest.astype(bf16)
    low = (rest - mid.astype(f32)).astype(bf16)
    return [hi, mid, low]


def partial_attend(query, key_ref, image_ref, w_k, w_v, out_ref):
    width = w_k.shape[1]
    size = width // HEADS
    query = (query * size ** (-0.5)).astype(bf16)
    keys = bdot(key_ref[...], w_k).astype(bf16)
    values = dot_at(w_v, image_ref[...], 0, 1).astype(bf16)
    ones = jnp.ones((size, values.shape[1]), bf16)
    totals, tops = [], []
    ahead = [dot_at(keys, one_head(query, head, size), 1, 1) for head in range(A1_AHEAD)]
    for head in range(HEADS):
        if head + A1_AHEAD < HEADS:
            ahead.append(dot_at(keys, one_head(query, head + A1_AHEAD, size), 1, 1))
        scores = ahead.pop(0)
        top = jnp.max(scores, axis=0, keepdims=True)
        weights = jnp.exp(scores - top).astype(bf16)
        own = values[head * size : (head + 1) * size]
        both = bdot(jnp.concatenate([own, ones], axis=0), weights)
        out_ref[head * size : (head + 1) * size, :] = both[:size].astype(bf16)
        totals.append(both[size : size + 1])
        tops.append(top)
    total = jnp.concatenate(totals, axis=0)
    tops = pieces(jnp.concatenate(tops, axis=0))
    tail = jnp.concatenate([total] + [t.astype(f32) for t in tops], axis=0)
    out_ref[width:, :] = tail.astype(bf16)


def first_kernel(tok_ref, image_ref, cols_ref, rows_ref, w_ref, out_ref, key_ref):
    step = 4
    for k in range(0, rows_ref.shape[0], step):
        at = slice(k * GRID, (k + step) * GRID)
        code = code_rows(cols_ref, rows_ref, k, step)
        key_ref[at, :] = (image_ref[at, :].astype(f32) + code).astype(bf16)
    query = bdot(tok_ref[...].astype(bf16), w_ref[0, 0]).astype(bf16)
    partial_attend(query.astype(f32), key_ref, image_ref, w_ref[0, 1], w_ref[0, 2], out_ref)


def token_kernel(
    layer, p0, p1, p2, p3, tok_ref, w_ref, up_ref, down_ref, out_ref, short_ref
):
    refs = (p0, p1, p2, p3)
    width = w_ref.shape[2]
    size = width // HEADS
    tails = [r[width:, :].astype(f32) for r in refs]
    tops = [t[HEADS : 2 * HEADS] + (t[2 * HEADS : 3 * HEADS] + t[3 * HEADS :]) for t in tails]
    peak = jnp.maximum(jnp.maximum(tops[0], tops[1]), jnp.maximum(tops[2], tops[3]))
    shares = [jnp.exp(t - peak) for t in tops]
    total = sum(t[:HEADS] * s for t, s in zip(tails, shares))
    heads = []
    for head in range(HEADS):
        at = slice(head * size, (head + 1) * size)
        row = slice(head, head + 1)
        summed = sum(r[at, :].astype(f32) * s[row] for r, s in zip(refs, shares))
        heads.append(summed / total[row])
    first = jnp.concatenate(heads, axis=0).astype(bf16)
    two = norm_rows(tok_ref[...] + dot_at(first, w_ref[layer, 0], 0, 0))
    hidden = jnp.maximum(bdot(two.astype(bf16), up_ref[layer]), 0.0).astype(bf16)
    three = norm_rows(two + bdot(hidden, down_ref[layer]))
    out_ref[...] = three
    short_ref[...] = three.astype(bf16)


def token_sides(tok_refs, scal_ref, w_k, w_v, k_ref, v_ref):
    width = w_k.shape[1]
    toks = tok_refs[0].shape[0]
    for k, ref in enumerate(tok_refs):
        at = slice(k * toks, (k + 1) * toks)
        tok = ref[...]
        first = (scal_ref[0] ^ k) * toks
        k_ref[at, :width] = bdot(tok, w_k).astype(bf16)
        row = lax.broadcasted_iota(jnp.int32, (toks, width), 0) + first
        lane = lax.broadcasted_iota(jnp.int32, (toks, width), 1)
        dead = (row >= scal_ref[1] * TOKS_P) & (lane == 0)
        k_ref[at, width:] = jnp.where(dead, -1e30, 0.0).astype(bf16)
        v_ref[:, at] = dot_at(w_v, tok, 0, 1).astype(bf16)


def image_attend(key, w_q, w_o, k_ref, v_ref, early):
    width = w_q.shape[1]
    size = width // HEADS
    query = bdot(key, w_q).astype(bf16).astype(f32) * size ** (-0.5)
    lane = lax.broadcasted_iota(jnp.int32, query.shape, 1)
    query = jnp.concatenate([query, jnp.where(lane == 0, 1.0, 0.0)], axis=1).astype(bf16)
    ones = jnp.ones((size, v_ref.shape[1]), bf16)


    def scores_of(head):
        own = one_head(k_ref[:, :width], head, size)
        return dot_at(jnp.concatenate([own, k_ref[:, width:]], axis=1), query, 1, 1)

    heads = []
    ahead = [scores_of(head) for head in range(early)]
    for head in range(HEADS):
        if head + early < HEADS:
            ahead.append(scores_of(head + early))
        scores = ahead.pop(0)
        top = jnp.max(scores, axis=0, keepdims=True)
        weights = jnp.exp(scores - top).astype(bf16)
        own = v_ref[head * size : (head + 1) * size, :]
        both = bdot(jnp.concatenate([own, ones], axis=0), weights)
        heads.append(both[:size] / both[size : size + 1])
    second = jnp.concatenate(heads, axis=0).astype(bf16)
    return dot_at(second, w_o, 0, 0)


def middle_kernel(
    scal_ref, t0, t1, t2, t3, image_ref, cols_ref, rows_ref, w_ref, o_ref,
    out_ref, own_ref, own_key_ref, k_ref, v_ref, key_ref, new_ref, full_ref,
):
    token_sides((t0, t1, t2, t3), scal_ref, w_ref[0, 4], w_ref[0, 5], k_ref, v_ref)
    step = 4
    for k in range(0, rows_ref.shape[0], step):
        at = slice(k * GRID, (k + step) * GRID)
        code = code_rows(cols_ref, rows_ref, k, step)
        full_ref[at, :] = code
        key_ref[at, :] = (image_ref[at, :].astype(f32) + code).astype(bf16)
    change = image_attend(key_ref[...], w_ref[0, 3], o_ref[0, 1], k_ref, v_ref, 1)
    image = norm_rows(image_ref[...].astype(f32) + change)
    new_ref[...] = image.astype(bf16)
    key_ref[...] = (image + full_ref[...]).astype(bf16)
    full_ref[...] = image
    own = pl.ds(pl.multiple_of(scal_ref[2], own_ref.shape[0]), own_ref.shape[0])
    own_ref[...] = full_ref[own, :]
    own_key_ref[...] = key_ref[own, :]
    query = bdot(t0[...], w_ref[1, 0]).astype(bf16)
    partial_attend(query.astype(f32), key_ref, new_ref, w_ref[1, 1], w_ref[1, 2], out_ref)


def last_kernel(
    scal_ref, t0, t1, t2, t3, image_ref, key_ref, w_ref, o_ref, hq_ref, hyper_ref,
    out_ref, k_ref, v_ref, logit_ref,
):
    refs = (t0, t1, t2, t3)
    token_sides(refs, scal_ref, w_ref[1, 4], w_ref[1, 5], k_ref, v_ref)
    image = image_ref[...]
    change = image_attend(key_ref[...], w_ref[1, 3], o_ref[1, 1], k_ref, v_ref, 4)
    image = norm_rows(image + change)
    feats = (image + hq_ref[...].astype(f32)).astype(bf16)
    scale = image.shape[1] ** (-0.5)
    toks = t0.shape[0]
    prompts = toks // TOKS_P
    for k, ref in enumerate(refs):
        hyper = bdot(ref[...], hyper_ref[...]).astype(bf16)
        logit_ref[...] = dot_at(hyper, feats, 1, 1) * scale
        rows = logit_ref[pl.ds(TOKS_P - 3, prompts, stride=TOKS_P), :]
        first = (scal_ref[0] ^ k) * prompts
        live = lax.broadcasted_iota(jnp.int32, rows.shape, 0) + first < scal_ref[1]
        out_ref[pl.ds(pl.multiple_of(first, prompts), prompts), :] = jnp.where(live, rows, 0.0)


def call(kernel, name, outs, scratch=(), scalars=0):
    vmem = pl.BlockSpec(memory_space=pltpu.VMEM)

    def run(*args):
        specs = [pl.BlockSpec(memory_space=pltpu.SMEM)] * scalars
        specs += [vmem] * (len(args) - scalars)
        return pl.pallas_call(
            kernel,
            out_shape=[jax.ShapeDtypeStruct(s, d) for s, d in outs],
            in_specs=specs,
            out_specs=[vmem] * len(outs),
            scratch_shapes=[pltpu.VMEM(s, d) for s, d in scratch],
            compiler_params=pltpu.CompilerParams(vmem_limit_bytes=20 * 2**20),
            name=name,
        )(*args)

    return run


def shards(
    early_feats,
    final_embed,
    prompt_counts,
    box_pixels,
    pair_table,
    token_table,
    pe_basis,
    w_early,
    attend_in,
    attend_out,
    mlp_up,
    mlp_down,
    w_hyper,
):
    images, pos_dev, width = final_embed.shape
    prompts = box_pixels.shape[1]
    n_x, n_zh, n_zl, n_y = (lax.axis_size(a) for a in IMG)
    section = lax.axis_index("section")
    my_x, my_zh, my_zl, my_y = (lax.axis_index(a) for a in IMG)
    mine = section * images + my_y

    sent = jnp.broadcast_to(final_embed[None], (n_x * n_zh,) + final_embed.shape)
    sent = sent.reshape(n_x * n_zh * n_y, pos_dev, width)
    held = lax.all_to_all(sent, ("x", "zh", "y"), 0, 0, tiled=True)
    image = held.reshape(-1, width)

    hq = jax.nn.gelu(bdot(early_feats, w_early), approximate=False).astype(bf16)
    hq_keep = lax.dynamic_index_in_dim(hq, my_y, 0, keepdims=False)
    hq_send = lax.dynamic_index_in_dim(hq, 1 - my_y, 0, keepdims=False)
    hq_got = swapped(hq_send, "y", 1)
    hq_here = jnp.where(
        my_y == 0,
        jnp.concatenate([hq_keep, hq_got], axis=0),
        jnp.concatenate([hq_got, hq_keep], axis=0),
    )

    ids = jnp.arange(n_x * n_zh * n_y, dtype=jnp.int32)
    grid_rows = (ids // 4) * (n_zh * n_zl * n_y) + (ids // 2 % 2) * (n_zl * n_y)
    grid_rows = grid_rows + my_zl * n_y + ids % 2
    cols, rows = grid_tables(grid_rows, pe_basis)
    rows = rows[:, None]
    count = prompt_counts[mine]
    boxes = lax.dynamic_index_in_dim(box_pixels, mine, 0, keepdims=False)
    own_prompts = prompts // n_x
    boxes = lax.dynamic_slice_in_dim(boxes, my_x * own_prompts, own_prompts, 0)
    tok = start_tokens(boxes, token_table, pe_basis)
    own_pos = n_y * pos_dev
    scal = jnp.stack([my_x, count, (my_x * n_zh + my_zh) * own_pos]).astype(jnp.int32)
    table = lax.dynamic_index_in_dim(pair_table, section * images, 0, keepdims=False)
    place = jnp.stack([(table // images) ^ section, table % images])
    tok, cols, rows, scal, place, hq_here = lax.optimization_barrier(
        (tok, cols, rows, scal, place, hq_here)
    )
    n_tok, n_pos, att = tok.shape[0], image.shape[0], attend_in.shape[-1]
    packed = ((att + 4 * HEADS, n_tok), bf16)
    sides = [((n_x * n_tok, 2 * att), bf16), ((att, n_x * n_tok), bf16)]

    def token_step(part, tok, layer):
        parts = [part] + [swapped(part, "zl", d) for d in range(1, n_zl)]
        outs = [(tok.shape, f32), (tok.shape, bf16)]
        tok, short = call(functools.partial(token_kernel, layer), "tokens", outs)(
            *parts, tok, attend_out, mlp_up, mlp_down
        )
        return tok, [short] + [swapped(short, "x", d) for d in range(1, n_x)]

    (part,) = call(first_kernel, "first", [packed], [((n_pos, width), bf16)])(
        tok, image, cols, rows, attend_in
    )
    tok, toks = token_step(part, tok, 0)
    part, own, own_key = call(
        middle_kernel,
        "middle",
        [packed, ((own_pos, width), f32), ((own_pos, width), bf16)],
        sides + [((n_pos, width), d) for d in (bf16, bf16, f32)],
        1,
    )(scal, *toks, image, cols, rows, attend_in, attend_out)
    tok, toks = token_step(part, tok, 1)
    (masks,) = call(
        last_kernel,
        "last",
        [((prompts, own_pos), f32)],
        sides + [((n_tok, own_pos), f32)],
        1,
    )(scal, *toks, own, own_key, attend_in, attend_out, hq_here, w_hyper)

    halves = [masks[:, :pos_dev], masks[:, pos_dev:]]
    keep = jnp.where(my_y == 0, halves[0], halves[1])
    give = jnp.where(my_y == 0, halves[1], halves[0])
    got = swapped(give, "y", 1)
    both = jnp.where(my_y == 0, jnp.stack([keep, got]), jnp.stack([got, keep]))
    every = jnp.stack(
        [both] + [swapped(both, "section", d) for d in range(1, lax.axis_size("section"))]
    )
    chosen = lax.dynamic_index_in_dim(every, place[0], 0, keepdims=False)
    swap = place[1] == 1
    return jnp.where(swap, chosen[::-1], chosen)


def solution(mesh):
    n_sec, n_img = mesh.devices.shape
    fine = Mesh(mesh.devices.reshape(n_sec, 4, 2, 4, 2), SPLIT)
    placed = (P("section", IMG, None),) * 2 + (P(),) * 11
    return jax.shard_map(
        shards, mesh=fine, in_specs=placed, out_specs=P("section", None, IMG), check_vma=False
    )
```
